512 devices in a mesh: site: 32 (over x, z), clade: 16 (over y, core).
Axes of the slice: x: 4, y: 8, z: 8, core: 2. Of those that a mesh axis runs over, the one named last changes fastest.
Arguments:
- tips: int32 [512, 131072], P('clade', 'site'), may hold values from 0 to 4
- transition: float32 [992, 4, 4, 4], P('clade'), may hold values from 0 to 1, as said below
- clade_children: int32 [496, 2], P('clade'), may hold values from 0 to 61, as said below
- upper_transition: float32 [30, 4, 4, 4], replicated, may hold values from 0 to 1, as said below
- upper_children: int32 [15, 2], replicated, may hold values from 0 to 29, as said below
- pattern_weights: int32 [131072], P('site'), may hold values from 1 to 8
Outputs:
- weighted_loglik: float32 [131072], P(('site', 'clade'))
- mean_loglik: float32 [], replicated
The draws below stay inside these ranges and needn't reach their ends.
Inputs may be any that keep to these rules, and one draw needn't show every extreme that they name: `tips`: code 4 marks a gap or an unknown base. `transition`: every row of every 4 x 4 block is positive and sums to 1. `upper_transition`: every row of every 4 x 4 block is positive and sums to 1. `clade_children`: rows k * (31) to (k + 1) * 31 - 1 belong to clade k; its row j holds two different node numbers below 32 + j, and each node 0 to 61 of the clade is a child in exactly one row of the clade. `upper_children`: row j holds two different node numbers below 16 + j, and each node 0 to 29 is a child in exactly one row.
All inputs are finite; a program needn't handle non-finite values.
Results may differ from the reference program's by a relative error of at most 0.0003.
Values sent between devices are 32-bit elements; how exact they have to be, the bound alone decides.
No kernel may reach another device: no remote copies, remote signals or barrier semaphores. Data moves between devices by JAX's collectives and lax.ppermute only.
A program may use at most 64 MiB of HBM per device.

```python
import jax
import jax.numpy as jnp
from jax import lax

LEAF = 32
RATES = 4
TAXA = 512
SITES = 131072
N_CLADE = 16


def tree_merges(base_key, leaf_count):
    active = jnp.arange(leaf_count, dtype=jnp.int32)
    merges = jnp.zeros((leaf_count - 1, 2), jnp.int32)

    def advance(node_index, state_pair):
        active_now, merges_now = state_pair
        live_count = leaf_count - node_index
        step_key = jax.random.fold_in(base_key, node_index)
        key_one, key_two = jax.random.split(step_key)
        first_pick = jax.random.randint(key_one, (), 0, live_count)
        second_pick = jax.random.randint(key_two, (), 0, live_count - 1)
        second_pick = jnp.where(second_pick >= first_pick, second_pick + 1, second_pick)
        pair_row = jnp.stack([active_now[first_pick], active_now[second_pick]]).astype(jnp.int32)
        merges_now = merges_now.at[node_index].set(pair_row)
        active_now = active_now.at[first_pick].set((leaf_count + node_index).astype(jnp.int32))
        active_now = active_now.at[second_pick].set(active_now[live_count - 1])
        return (active_now, merges_now)
    return lax.fori_loop(0, leaf_count - 1, advance, (active, merges))[1]


def stochastic(base_key, edge_count):
    key_one, key_two = jax.random.split(base_key)
    lengths = jnp.exp(jax.random.uniform(key_one, (edge_count, RATES, 1, 1), jnp.float32, jnp.log(0.03), jnp.log(0.6)))
    roughness = jax.random.uniform(key_two, (edge_count, RATES, 4, 4), jnp.float32, 0.3, 1.0)
    identity = jnp.eye(4, dtype=jnp.float32)
    raw_rates = identity + lengths * roughness * (1.0 - identity)
    return raw_rates / jnp.sum(raw_rates, axis=-1, keepdims=True)


def draw_transition(key, part):
    return stochastic(jax.random.fold_in(key, 21), (2 * LEAF - 2) * N_CLADE)


def draw_upper_transition(key, part):
    return stochastic(jax.random.fold_in(key, 22), 2 * N_CLADE - 2)


def draw_clade_children(key, part):
    clade_keys = jax.random.split(jax.random.fold_in(key, 11), N_CLADE)
    merged = jax.vmap(lambda subkey: tree_merges(subkey, LEAF))(clade_keys)
    return merged.reshape((N_CLADE * (LEAF - 1), 2))


def draw_upper_children(key, part):
    return tree_merges(jax.random.fold_in(key, 12), N_CLADE)


def plant(array, rng, least, top_value):
    place = [jax.random.randint(jax.random.fold_in(rng, axis), (), 0, length) for axis, length in enumerate(array.shape)]
    widest = array.shape.index(max(array.shape))
    next_to = place[:widest] + [(place[widest] + 1) % array.shape[widest]] + place[widest + 1:]
    return array.at[tuple(place)].set(least).at[tuple(next_to)].set(top_value)


def setup_inputs(seed: int = 0) -> dict:
    arg_keys = jax.random.split(jax.random.key(seed), 7)
    return {
        "tips": plant(jax.random.randint(arg_keys[0], (TAXA, SITES), 0, 5), jax.random.fold_in(arg_keys[0], 1), 0, 4).astype(jnp.int32),
        "transition": draw_transition(jax.random.fold_in(arg_keys[6], 71), 0),
        "clade_children": draw_clade_children(jax.random.fold_in(arg_keys[6], 71), 0),
        "upper_transition": draw_upper_transition(jax.random.fold_in(arg_keys[6], 71), 0),
        "upper_children": draw_upper_children(jax.random.fold_in(arg_keys[6], 71), 0),
        "pattern_weights": plant(jax.random.randint(arg_keys[5], (SITES,), 1, 9), jax.random.fold_in(arg_keys[5], 1), 1, 8).astype(jnp.int32),
    }


def transform(matrix, values_in):
    return jnp.einsum("rab,rbs->ras", matrix, values_in, precision=lax.Precision.HIGHEST)


def prune_tree(partials, scales, matrices, merges, first_new):
    def advance(node_index, state_pair):
        cur_parts, cur_scales = state_pair
        left_index = merges[node_index, 0]
        right_index = merges[node_index, 1]
        product = transform(matrices[left_index], cur_parts[left_index]) * transform(matrices[right_index], cur_parts[right_index])
        biggest = jnp.max(product, axis=(0, 1))
        new_scale = cur_scales[left_index] + cur_scales[right_index] + jnp.log(biggest)
        target = (first_new + node_index).astype(jnp.int32)
        cur_parts = lax.dynamic_update_index_in_dim(cur_parts, product / biggest, target, 0)
        cur_scales = lax.dynamic_update_index_in_dim(cur_scales, new_scale, target, 0)
        return cur_parts, cur_scales

    return lax.fori_loop(0, merges.shape[0], advance, (partials, scales))


def tip_partials(tip_codes, rate_count):
    states = jnp.arange(4, dtype=jnp.int32)
    matches = (tip_codes[:, None, :] == states[None, :, None]) | (tip_codes[:, None, :] == 4)
    single = matches.astype(jnp.float32)
    return jnp.broadcast_to(single[:, None], (single.shape[0], rate_count, 4, single.shape[2]))


def clade_root(tip_codes, matrices, merges):
    leaf_count = tip_codes.shape[0]
    site_count = tip_codes.shape[1]
    rate_count = matrices.shape[1]
    leaves = tip_partials(tip_codes, rate_count)
    partials = jnp.concatenate([leaves, jnp.zeros((leaf_count - 1, rate_count, 4, site_count), jnp.float32)], axis=0)
    scales = jnp.zeros((2 * leaf_count - 1, site_count), jnp.float32)
    partials, scales = prune_tree(partials, scales, matrices, merges, leaf_count)
    return partials[-1], scales[-1]


def upper_root(root_parts, root_scales, matrices, merges):
    clade_total = root_parts.shape[0]
    partials = jnp.concatenate([root_parts, jnp.zeros((clade_total - 1,) + root_parts.shape[1:], jnp.float32)], axis=0)
    scales = jnp.concatenate([root_scales, jnp.zeros((clade_total - 1, root_scales.shape[1]), jnp.float32)], axis=0)
    partials, scales = prune_tree(partials, scales, matrices, merges, clade_total)
    return partials[-1], scales[-1]


def site_loglik(root_part, root_scale, weights, taxa_total):
    summed = jnp.sum(root_part, axis=(0, 1)) / (4.0 * root_part.shape[0])
    return weights.astype(jnp.float32) * (jnp.log(summed) + root_scale) / taxa_total


def reference(tips, transition, clade_children, upper_transition, upper_children, pattern_weights):
    edge_count = 2 * LEAF - 2

    def one_clade(clade_index):
        tip_codes = lax.dynamic_slice_in_dim(tips, clade_index * LEAF, LEAF, 0)
        matrices = lax.dynamic_slice_in_dim(transition, clade_index * edge_count, edge_count, 0)
        merges = lax.dynamic_slice_in_dim(clade_children, clade_index * (LEAF - 1), LEAF - 1, 0)
        return clade_root(tip_codes, matrices, merges)

    root_parts, root_scales = lax.map(one_clade, jnp.arange(N_CLADE, dtype=jnp.int32))
    final_part, final_scale = upper_root(root_parts, root_scales, upper_transition, upper_children)
    weighted = site_loglik(final_part, final_scale, pattern_weights, float(LEAF * N_CLADE))
    return weighted, jnp.sum(weighted) / SITES
```

```python
import jax
import jax.numpy as jnp
from jax import lax
from jax.experimental import pallas as pl
from jax.experimental.pallas import tpu as pltpu
from jax.sharding import Mesh
from jax.sharding import PartitionSpec as P

CLADE = ("clade_0", "clade_1")
SITE = ("site_0", "site_1")
SITE_CLADE = SITE + CLADE


def splat(column_block, k):
    return jnp.broadcast_to(column_block[:, k : k + 1], (8, 128))


def clade_kernel(merges_ref, probs_ref, tips_ref, tables_ref, out_ref, parts_ref, inv_ref, log_ref):
    merges = merges_ref.shape[0] // 2
    leaves = merges + 1
    groups = out_ref.shape[0] // 32
    tiles = range(2 * groups // 8)
    log_ref[...] = jnp.zeros_like(log_ref)

    def codes(taxon):
        start = (taxon // 8) * (16 * groups) + taxon % 8
        halves = [tips_ref[pl.ds(start + 8 * h, groups, stride=16), :] for h in range(2)]
        return [half[8 * i : 8 * i + 8] for half in halves for i in range(groups // 8)]

    def leaf_branch(taxon):
        idx = codes(taxon)
        table = tables_ref[taxon]

        def planes(rate):
            for state in range(4):
                column = splat(table, rate * 4 + state)
                yield [
                    jnp.take_along_axis(column, idx[t], axis=0, mode="promise_in_bounds")
                    for t in tiles
                ]

        return planes

    def inner_branch(node):
        inner = node - leaves
        inv = [inv_ref[inner, 8 * t : 8 * t + 8, :] for t in tiles]

        def planes(rate):
            part = [
                [
                    parts_ref[inner * 16 + rate * 4 + b, 8 * t : 8 * t + 8, :] * inv[t]
                    for t in tiles
                ]
                for b in range(4)
            ]
            for state in range(4):
                p = [probs_ref[node * 64 + rate * 16 + state * 4 + b] for b in range(4)]
                yield [
                    (p[0] * part[0][t] + p[1] * part[1][t])
                    + (p[2] * part[2][t] + p[3] * part[3][t])
                    for t in tiles
                ]

        return planes

    def combine(j, one, other, keep):
        biggest = None
        for rate in range(4):
            for state, (u, v) in enumerate(zip(one(rate), other(rate))):
                q = [u[t] * v[t] for t in tiles]
                keep(rate, state, q)
                biggest = q if biggest is None else [jnp.maximum(biggest[t], q[t]) for t in tiles]
        return biggest

    def merge(j, high, low):
        def keep(rate, state, q):
            for t in tiles:
                parts_ref[j * 16 + rate * 4 + state, 8 * t : 8 * t + 8, :] = q[t]

        def run(one, other):
            biggest = combine(j, one(high), other(low), keep)
            for t in tiles:
                rows = slice(8 * t, 8 * t + 8)
                inv = pl.reciprocal(biggest[t], approx=True)
                inv_ref[j, rows, :] = inv
                log_ref[rows, :] = log_ref[rows, :] - jnp.log(inv)

        pl.when(high < leaves)(lambda: run(leaf_branch, leaf_branch))
        pl.when((high >= leaves) & (low < leaves))(lambda: run(inner_branch, leaf_branch))
        pl.when(low >= leaves)(lambda: run(inner_branch, inner_branch))

    def step(j, _):
        c, d = merges_ref[2 * j], merges_ref[2 * j + 1]
        merge(j, jnp.maximum(c, d), jnp.minimum(c, d))
        return 0

    lax.fori_loop(0, merges, step, 0)

    last = merges - 1
    for t in tiles:
        rows = slice(8 * t, 8 * t + 8)
        h, first = divmod(8 * t, groups)
        scale = log_ref[rows, :] + jnp.log(inv_ref[last, rows, :])
        for rate in range(4):
            for state in range(4):
                value = jnp.log(parts_ref[last * 16 + rate * 4 + state, rows, :]) + scale
                out_ref[pl.ds(first * 32 + state * 8 + rate * 2 + h, 8, stride=32), :] = value


def upper_kernel(total_taxa, merges_ref, roots_ref, probs_ref, weights_ref, out_ref, sum_ref, parts_ref):
    merges = merges_ref.shape[0] // 2
    clades = merges + 1

    def over_rates(op, x):
        x = op(x, pltpu.roll(x, 2, 0))
        return op(x, pltpu.roll(x, 4, 0))

    scale = jnp.zeros((8, 128), jnp.float32)
    for k in range(clades):
        rows = [roots_ref[k * 32 + 8 * a : k * 32 + 8 * a + 8, :] for a in range(4)]
        top = jnp.maximum(jnp.maximum(rows[0], rows[1]), jnp.maximum(rows[2], rows[3]))
        top = over_rates(jnp.maximum, top)
        scale = scale + top
        for a in range(4):
            parts_ref[k, 8 * a : 8 * a + 8, :] = jnp.exp(rows[a] - top)

    def branch(node):
        part = [parts_ref[node, 8 * b : 8 * b + 8, :] for b in range(4)]
        block = probs_ref[node]
        out = []
        for a in range(4):
            p = [splat(block, a * 4 + b) for b in range(4)]
            out.append((p[0] * part[0] + p[1] * part[1]) + (p[2] * part[2] + p[3] * part[3]))
        return out

    for j in range(merges):
        u, v = branch(merges_ref[2 * j]), branch(merges_ref[2 * j + 1])
        q = [u[a] * v[a] for a in range(4)]
        if j < merges - 1:
            top = jnp.maximum(jnp.maximum(q[0], q[1]), jnp.maximum(q[2], q[3]))
            inv = pl.reciprocal(over_rates(jnp.maximum, top), approx=True)
            scale = scale - jnp.log(inv)
            for a in range(4):
                parts_ref[clades + j, 8 * a : 8 * a + 8, :] = q[a] * inv
        else:
            top = over_rates(jnp.maximum, jnp.maximum(jnp.maximum(q[0], q[1]), jnp.maximum(q[2], q[3])))
            inv = pl.reciprocal(top, approx=True)
            scale = scale - jnp.log(inv)
            total = over_rates(jnp.add, ((q[0] + q[1]) + (q[2] + q[3])) * inv)
    loglik = (jnp.log(total * (1.0 / 16.0)) + scale)[0:2, :]
    weighted = weights_ref[...].astype(jnp.float32) * loglik * (1.0 / total_taxa)
    out_ref[...] = weighted
    sum_ref[...] = jnp.broadcast_to(weighted[0:1, :] + weighted[1:2, :], sum_ref.shape)


def sum_over(rows, axes, copies):
    got = lax.all_to_all(rows, axes, split_axis=0, concat_axis=0, tiled=True)
    return jnp.broadcast_to(jnp.sum(got, axis=0, keepdims=True), (copies,) + got.shape[1:])


def per_device(tips, transition, clade_children, upper_transition, upper_children, pattern_weights):
    leaves, sites = tips.shape
    clades = lax.axis_size(CLADE)
    groups = lax.axis_size(SITE)
    position = lax.axis_index(CLADE)
    piece = sites // clades
    nodes = transition.shape[0]
    vmem = pl.BlockSpec(memory_space=pltpu.VMEM)
    smem = pl.BlockSpec(memory_space=pltpu.SMEM)

    tiled = tips.reshape(leaves // 8, 8, sites // 128, 128).transpose(0, 2, 1, 3)
    tiled = tiled.reshape(leaves * sites // 128, 128)
    by_code = transition[:leaves].reshape(leaves, 16, 4)
    gap = jnp.sum(by_code, axis=2, keepdims=True)
    tables = jnp.concatenate([by_code, gap, jnp.zeros((leaves, 16, 3), jnp.float32)], axis=2)
    tables = tables.transpose(0, 2, 1)
    logs = pl.pallas_call(
        clade_kernel,
        out_shape=jax.ShapeDtypeStruct((clades * 32, 128), jnp.float32),
        in_specs=[smem, smem, vmem, vmem],
        out_specs=vmem,
        scratch_shapes=[
            pltpu.VMEM(((leaves - 1) * 16, sites // 128, 128), jnp.float32),
            pltpu.VMEM((leaves - 1, sites // 128, 128), jnp.float32),
            pltpu.VMEM((sites // 128, 128), jnp.float32),
        ],
        name="clade",
    )(clade_children.reshape(-1), transition.reshape(-1), tiled, tables)

    got = lax.all_to_all(
        logs.reshape(clades, 32, 128), CLADE, split_axis=0, concat_axis=0, tiled=True
    )
    upper = upper_transition.reshape(-1, 4, 16)
    upper = jnp.repeat(upper, 2, axis=1)
    own = lax.dynamic_slice_in_dim(pattern_weights, position * piece, piece, 0)
    weighted, addend = pl.pallas_call(
        lambda *refs: upper_kernel(float(leaves * clades), *refs),
        out_shape=[
            jax.ShapeDtypeStruct((piece // 128, 128), jnp.float32),
            jax.ShapeDtypeStruct((clades, 128), jnp.float32),
        ],
        in_specs=[smem, vmem, vmem, vmem],
        out_specs=[vmem, vmem],
        scratch_shapes=[pltpu.VMEM((2 * clades - 1, 32, 128), jnp.float32)],
        name="upper",
    )(upper_children.reshape(-1), got.reshape(clades * 32, 128), upper, own.reshape(piece // 128, 128))

    part = sum_over(addend.reshape(clades, 1, 128), CLADE, groups)
    whole = sum_over(part, SITE, 1)
    return weighted.reshape(piece), jnp.sum(whole) / (sites * groups)


def solution(mesh):
    torus = Mesh(mesh.devices.reshape(4, 8, 8, 2), SITE_CLADE)
    return jax.shard_map(
        per_device,
        mesh=torus,
        in_specs=(P(CLADE, SITE), P(CLADE, None, None, None), P(CLADE, None), P(), P(), P(SITE)),
        out_specs=(P(SITE_CLADE), P()),
        check_vma=False,
    )
```

```python
import jax
import jax.numpy as jnp
from jax import lax
from jax.experimental import pallas as pl
from jax.experimental.pallas import tpu as pltpu
from jax.sharding import Mesh
from jax.sharding import PartitionSpec as P

CLADE = ("clade_0", "clade_1")
SITE = ("site_0", "site_1")
SITE_CLADE = SITE + CLADE


def splat(column_block, k):
    return jnp.broadcast_to(column_block[:, k : k + 1], (8, 128))


def by_row(rows):
    shape = (8, rows[0].shape[1])
    sublane = lax.broadcasted_iota(jnp.int32, shape, 0)
    block = jnp.broadcast_to(rows[-1], shape)
    for s in reversed(range(len(rows) - 1)):
        block = jnp.where(sublane <= s, jnp.broadcast_to(rows[s], shape), block)
    return block


def clade_kernel(
    merges_hbm, rows_hbm, tips_hbm, out_hbm,
    merges_ref, probs_ref, rows_ref, tips_ref, tables_ref, parts_ref, inv_ref, log_ref, root_ref, sems,
):
    copies = [
        pltpu.make_async_copy(source, target, sems.at[i])
        for i, (source, target) in enumerate(
            [(rows_hbm, rows_ref), (merges_hbm, merges_ref), (rows_hbm, probs_ref), (tips_hbm, tips_ref)]
        )
    ]
    for copy in copies:
        copy.start()
    merges = merges_ref.shape[1]
    leaves = merges + 1
    groups = out_hbm.shape[0] // 32
    tiles = range(2 * groups // 8)
    log_ref[...] = jnp.zeros_like(log_ref)
    copies[0].wait()
    blocks = []
    for k in range(16):
        rows = [rows_ref[4 * k + b : 4 * k + b + 1, :] for b in range(4)]
        blocks.append(by_row(rows + [(rows[0] + rows[1]) + (rows[2] + rows[3])]))
    for taxon in range(leaves):
        for k in range(16):
            tables_ref[taxon * 16 + k] = splat(blocks[k], taxon)
    for copy in copies[1:]:
        copy.wait()

    def codes(taxon):
        start = (taxon // 8) * (16 * groups) + taxon % 8
        halves = [tips_ref[pl.ds(start + 8 * h, groups, stride=16), :] for h in range(2)]
        return [half[8 * i : 8 * i + 8] for half in halves for i in range(groups // 8)]

    def leaf_branch(taxon):
        idx = codes(taxon)

        def planes(rate):
            for state in range(4):
                column = tables_ref[taxon * 16 + rate * 4 + state]
                yield [
                    jnp.take_along_axis(column, idx[t], axis=0, mode="promise_in_bounds")
                    for t in tiles
                ]

        return planes

    def inner_branch(node):
        inner = node - leaves
        inv = [inv_ref[inner, 8 * t : 8 * t + 8, :] for t in tiles]

        def planes(rate):
            part = [
                [
                    parts_ref[inner * 16 + rate * 4 + b, 8 * t : 8 * t + 8, :] * inv[t]
                    for t in tiles
                ]
                for b in range(4)
            ]
            for state in range(4):
                p = [probs_ref[rate * 16 + state * 4 + b, node] for b in range(4)]
                yield [
                    (p[0] * part[0][t] + p[1] * part[1][t])
                    + (p[2] * part[2][t] + p[3] * part[3][t])
                    for t in tiles
                ]

        return planes

    def merge(j, one, other):
        biggest = None
        for rate in range(4):
            firsts = list(one(rate))
            for state, (u, v) in enumerate(zip(firsts, other(rate))):
                q = [u[t] * v[t] for t in tiles]
                for t in tiles:
                    parts_ref[j * 16 + rate * 4 + state, 8 * t : 8 * t + 8, :] = q[t]
                biggest = q if biggest is None else [jnp.maximum(biggest[t], q[t]) for t in tiles]
        for t in tiles:
            rows = slice(8 * t, 8 * t + 8)
            inv = pl.reciprocal(biggest[t], approx=True)
            inv_ref[j, rows, :] = inv
            log_ref[rows, :] = log_ref[rows, :] - jnp.log(inv)

    def step(j, _):
        c, d = merges_ref[0, j], merges_ref[1, j]
        leaf, inner = leaf_branch, inner_branch
        high, low = jnp.maximum(c, d), jnp.minimum(c, d)
        pl.when(high < leaves)(lambda: merge(j, leaf(high), leaf(low)))
        pl.when((high >= leaves) & (low < leaves))(lambda: merge(j, inner(high), leaf(low)))
        pl.when(low >= leaves)(lambda: merge(j, inner(high), inner(low)))
        return 0

    lax.fori_loop(0, merges, step, 0)

    last = merges - 1
    half = 8 * 32
    sends = []
    for part in range(groups // 8):
        for h in range(2):
            rows = slice(h * groups + 8 * part, h * groups + 8 * part + 8)
            scale = log_ref[rows, :] + jnp.log(inv_ref[last, rows, :])
            for rate in range(4):
                for state in range(4):
                    value = jnp.log(parts_ref[last * 16 + rate * 4 + state, rows, :]) + scale
                    start = part * half + state * 8 + rate * 2 + h
                    root_ref[pl.ds(start, 8, stride=32), :] = value
        span = pl.ds(part * half, half)
        sends.append(pltpu.make_async_copy(root_ref.at[span], out_hbm.at[span], sems.at[4 + part]))
        sends[-1].start()
    for send in sends:
        send.wait()


def spread_kernel(rows_ref, out_ref):
    for k in range(16):
        rows = [rows_ref[16 * rate + k : 16 * rate + k + 1, :] for rate in range(4)]
        block = by_row([row for row in rows for _ in range(2)])
        for node in range(rows_ref.shape[1]):
            out_ref[node * 16 + k] = splat(block, node)


def upper_kernel(total_taxa, merges_ref, roots_ref, probs_ref, weights_ref, out_ref, sum_ref, parts_ref):
    merges = merges_ref.shape[1]
    clades = merges + 1

    def over_rates(op, x):
        x = op(x, pltpu.roll(x, 2, 0))
        return op(x, pltpu.roll(x, 4, 0))

    scale = jnp.zeros((8, 128), jnp.float32)
    for k in range(clades):
        rows = [roots_ref[k * 32 + 8 * a : k * 32 + 8 * a + 8, :] for a in range(4)]
        top = jnp.maximum(jnp.maximum(rows[0], rows[1]), jnp.maximum(rows[2], rows[3]))
        top = over_rates(jnp.maximum, top)
        scale = scale + top
        for a in range(4):
            parts_ref[k, 8 * a : 8 * a + 8, :] = jnp.exp(rows[a] - top)

    def branch(node):
        part = [parts_ref[node, 8 * b : 8 * b + 8, :] for b in range(4)]
        out = []
        for a in range(4):
            p = [probs_ref[node * 16 + a * 4 + b] for b in range(4)]
            out.append((p[0] * part[0] + p[1] * part[1]) + (p[2] * part[2] + p[3] * part[3]))
        return out

    for j in range(merges):
        u, v = branch(merges_ref[0, j]), branch(merges_ref[1, j])
        q = [u[a] * v[a] for a in range(4)]
        if j < merges - 1:
            top = jnp.maximum(jnp.maximum(q[0], q[1]), jnp.maximum(q[2], q[3]))
            inv = pl.reciprocal(over_rates(jnp.maximum, top), approx=True)
            scale = scale - jnp.log(inv)
            for a in range(4):
                parts_ref[clades + j, 8 * a : 8 * a + 8, :] = q[a] * inv
        else:
            top = over_rates(jnp.maximum, jnp.maximum(jnp.maximum(q[0], q[1]), jnp.maximum(q[2], q[3])))
            inv = pl.reciprocal(top, approx=True)
            scale = scale - jnp.log(inv)
            total = over_rates(jnp.add, ((q[0] + q[1]) + (q[2] + q[3])) * inv)
    loglik = (jnp.log(total * (1.0 / 16.0)) + scale)[0:2, :]
    weighted = weights_ref[...].astype(jnp.float32) * loglik * (1.0 / total_taxa)
    out_ref[...] = weighted
    sum_ref[...] = jnp.broadcast_to(weighted[0:1, :] + weighted[1:2, :], sum_ref.shape)


def sum_over(rows, axes, copies):
    got = lax.all_to_all(rows, axes, split_axis=0, concat_axis=0, tiled=True)
    return jnp.broadcast_to(jnp.sum(got, axis=0, keepdims=True), (copies,) + got.shape[1:])


def per_device(tips, transition, clade_children, upper_transition, upper_children, pattern_weights):
    leaves, sites = tips.shape
    clades = lax.axis_size(CLADE)
    groups = lax.axis_size(SITE)
    position = lax.axis_index(CLADE)
    piece = sites // clades
    nodes = transition.shape[0]
    vmem = pl.BlockSpec(memory_space=pltpu.VMEM)
    smem = pl.BlockSpec(memory_space=pltpu.SMEM)

    tiled = tips.reshape(leaves // 8, 8, sites // 128, 128).transpose(0, 2, 1, 3)
    tiled = tiled.reshape(leaves * sites // 128, 128)
    rows = transition.transpose(1, 2, 3, 0).reshape(64, -1)
    hbm = pl.BlockSpec(memory_space=pl.ANY)
    merges = clade_children.T
    logs = pl.pallas_call(
        clade_kernel,
        out_shape=jax.ShapeDtypeStruct((clades * 32, 128), jnp.float32),
        in_specs=[hbm, hbm, hbm],
        out_specs=hbm,
        scratch_shapes=[
            pltpu.SMEM(merges.shape, jnp.int32),
            pltpu.SMEM(rows.shape, jnp.float32),
            pltpu.VMEM(rows.shape, jnp.float32),
            pltpu.VMEM(tiled.shape, jnp.int32),
            pltpu.VMEM((leaves * 16, 8, 128), jnp.float32),
            pltpu.VMEM(((leaves - 1) * 16, sites // 128, 128), jnp.float32),
            pltpu.VMEM((leaves - 1, sites // 128, 128), jnp.float32),
            pltpu.VMEM((sites // 128, 128), jnp.float32),
            pltpu.VMEM((clades * 32, 128), jnp.float32),
            pltpu.SemaphoreType.DMA((6,)),
        ],
        name="clade",
    )(merges, rows, tiled)

    got = lax.all_to_all(
        logs.reshape(clades, 32, 128), CLADE, split_axis=0, concat_axis=0, tiled=True
    )
    upper_rows = upper_transition.transpose(1, 2, 3, 0).reshape(64, -1)
    spread = pl.pallas_call(
        spread_kernel,
        out_shape=jax.ShapeDtypeStruct((upper_rows.shape[1] * 16, 8, 128), jnp.float32),
        in_specs=[vmem],
        out_specs=vmem,
        compiler_params=pltpu.CompilerParams(vmem_limit_bytes=8 << 20),
        cost_estimate=pl.CostEstimate(flops=1 << 22, bytes_accessed=2 << 20, transcendentals=0),
        name="spread",
    )(upper_rows)
    own = lax.dynamic_slice_in_dim(pattern_weights, position * piece, piece, 0)
    weighted, addend = pl.pallas_call(
        lambda *refs: upper_kernel(float(leaves * clades), *refs),
        out_shape=[
            jax.ShapeDtypeStruct((piece // 128, 128), jnp.float32),
            jax.ShapeDtypeStruct((clades, 128), jnp.float32),
        ],
        in_specs=[smem, vmem, vmem, vmem],
        out_specs=[vmem, vmem],
        scratch_shapes=[pltpu.VMEM((2 * clades - 1, 32, 128), jnp.float32)],
        compiler_params=pltpu.CompilerParams(vmem_limit_bytes=8 << 20),
        name="upper",
    )(upper_children.T, got.reshape(clades * 32, 128), spread, own.reshape(piece // 128, 128))

    part = sum_over(addend.reshape(clades, 1, 128), CLADE, groups)
    whole = sum_over(part, SITE, 1)
    return weighted.reshape(piece), jnp.sum(whole) / (sites * groups)


def solution(mesh):
    torus = Mesh(mesh.devices.reshape(4, 8, 8, 2), SITE_CLADE)
    return jax.shard_map(
        per_device,
        mesh=torus,
        in_specs=(P(CLADE, SITE), P(CLADE, None, None, None), P(CLADE, None), P(), P(), P(SITE)),
        out_specs=(P(SITE_CLADE), P()),
        check_vma=False,
    )
```

```python
import jax
import jax.numpy as jnp
from jax import lax
from jax.experimental import pallas as pl
from jax.experimental.pallas import tpu as pltpu
from jax.sharding import Mesh
from jax.sharding import PartitionSpec as P

CLADE = "clade"
SITE = "site"
SITE_CLADE = (SITE, CLADE)
CLADE_FIRST = 8
SITE_FIRST = 20


def all_to_all(blocks, axis, first):
    members = lax.axis_size(axis)
    group = [(first + i) % members for i in range(members)]
    return lax.all_to_all(
        blocks, axis, split_axis=0, concat_axis=0, axis_index_groups=[group], tiled=True
    )


def splat(column_block, k):
    return jnp.broadcast_to(column_block[:, k : k + 1], (8, 128))


def by_row(rows):
    shape = (8, rows[0].shape[1])
    sublane = lax.broadcasted_iota(jnp.int32, shape, 0)
    block = jnp.broadcast_to(rows[-1], shape)
    for s in reversed(range(len(rows) - 1)):
        block = jnp.where(sublane <= s, jnp.broadcast_to(rows[s], shape), block)
    return block


def clade_kernel(
    merges_hbm, rows_hbm, tips_hbm, out_hbm,
    merges_ref, order_ref, probs_ref, rows_ref, tips_ref, tables_ref, parts_ref, top_ref, log_ref, root_ref, sems,
):
    copies = [
        pltpu.make_async_copy(source, target, sems.at[i])
        for i, (source, target) in enumerate(
            [(rows_hbm, rows_ref), (merges_hbm, merges_ref), (rows_hbm, probs_ref), (tips_hbm, tips_ref)]
        )
    ]
    for copy in copies:
        copy.start()
    merges = merges_ref.shape[1]
    leaves = merges + 1
    groups = out_hbm.shape[0] // 32
    tiles = range(2 * groups // 8)
    log_ref[...] = jnp.zeros_like(log_ref)
    copies[0].wait()
    copies[1].wait()
    blocks = []
    for k in range(16):
        rows = [rows_ref[4 * k + b : 4 * k + b + 1, :] for b in range(4)]
        blocks.append(by_row(rows + [(rows[0] + rows[1]) + (rows[2] + rows[3])]))
    for taxon in range(leaves):
        for k in range(16):
            tables_ref[taxon * 16 + k] = splat(blocks[k], taxon)
    pairs, others = jnp.int32(0), jnp.int32(0)
    for j in range(merges):
        is_pair = jnp.maximum(merges_ref[0, j], merges_ref[1, j]) < leaves
        order_ref[0, pairs] = j
        order_ref[1, others] = j
        pairs = pairs + jnp.where(is_pair, 1, 0)
        others = others + jnp.where(is_pair, 0, 1)
    copies[3].wait()

    def codes(taxon):
        start = (taxon // 8) * (16 * groups) + taxon % 8
        halves = [tips_ref[pl.ds(start + 8 * h, groups, stride=16), :] for h in range(2)]
        return [half[8 * i : 8 * i + 8] for half in halves for i in range(groups // 8)]

    def leaf_branch(taxon):
        idx = codes(taxon)

        def planes(rate):
            for state in range(4):
                column = tables_ref[taxon * 16 + rate * 4 + state]
                yield [
                    jnp.take_along_axis(column, idx[t], axis=0, mode="promise_in_bounds")
                    for t in tiles
                ]

        return planes

    def add_logs(invs):
        for t in tiles:
            rows = slice(8 * t, 8 * t + 8)
            log_ref[rows, :] = log_ref[rows, :] - sum(jnp.log(inv[t]) for inv in invs)

    def inner_branch(node):
        inner = node - leaves
        inv = [
            pl.reciprocal(top_ref[inner, 8 * t : 8 * t + 8, :], approx=True) for t in tiles
        ]

        def planes(rate):
            part = [
                [
                    parts_ref[inner * 16 + rate * 4 + b, 8 * t : 8 * t + 8, :] * inv[t]
                    for t in tiles
                ]
                for b in range(4)
            ]
            for state in range(4):
                p = [probs_ref[rate * 16 + state * 4 + b, node] for b in range(4)]
                yield [
                    (p[0] * part[0][t] + p[1] * part[1][t])
                    + (p[2] * part[2][t] + p[3] * part[3][t])
                    for t in tiles
                ]

        planes.inv = inv
        return planes

    def merge(j, one, other):
        add_logs_of = [branch.inv for branch in (one, other) if hasattr(branch, "inv")]
        if add_logs_of:
            add_logs(add_logs_of)
        biggest = None
        for rate in range(4):
            firsts = list(one(rate))
            for state, (u, v) in enumerate(zip(firsts, other(rate))):
                q = [u[t] * v[t] for t in tiles]
                for t in tiles:
                    parts_ref[j * 16 + rate * 4 + state, 8 * t : 8 * t + 8, :] = q[t]
                biggest = q if biggest is None else [jnp.maximum(biggest[t], q[t]) for t in tiles]
        for t in tiles:
            top_ref[j, 8 * t : 8 * t + 8, :] = biggest[t]

    def two_pairs(i, _):
        for place in (2 * i, jnp.minimum(2 * i + 1, pairs - 1)):
            j = order_ref[0, place]
            merge(j, leaf_branch(merges_ref[0, j]), leaf_branch(merges_ref[1, j]))
        return 0

    def step(i, _):
        j = order_ref[1, i]
        c, d = merges_ref[0, j], merges_ref[1, j]
        high, low = jnp.maximum(c, d), jnp.minimum(c, d)
        leaf, inner = leaf_branch, inner_branch
        pl.when(low < leaves)(lambda: merge(j, inner(high), leaf(low)))
        pl.when(low >= leaves)(lambda: merge(j, inner(high), inner(low)))
        return 0

    lax.fori_loop(0, (pairs + 1) // 2, two_pairs, 0)
    copies[2].wait()
    lax.fori_loop(0, others, step, 0)

    last = merges - 1
    half = 8 * 32
    sends = []
    for part in range(groups // 8):
        place = (part - CLADE_FIRST // 8) % (groups // 8)
        for h in range(2):
            rows = slice(h * groups + 8 * part, h * groups + 8 * part + 8)
            scale = log_ref[rows, :]
            for rate in range(4):
                for state in range(4):
                    value = jnp.log(parts_ref[last * 16 + rate * 4 + state, rows, :]) + scale
                    start = place * half + state * 8 + rate * 2 + h
                    root_ref[pl.ds(start, 8, stride=32), :] = value
        span = pl.ds(place * half, half)
        sends.append(pltpu.make_async_copy(root_ref.at[span], out_hbm.at[span], sems.at[4 + part]))
        sends[-1].start()
    for send in sends:
        send.wait()


def spread_kernel(rows_ref, out_ref):
    for k in range(16):
        rows = [rows_ref[16 * rate + k : 16 * rate + k + 1, :] for rate in range(4)]
        block = by_row([row for row in rows for _ in range(2)])
        for node in range(rows_ref.shape[1]):
            out_ref[node * 16 + k] = splat(block, node)


def upper_kernel(total_taxa, merges_ref, roots_ref, probs_ref, weights_ref, out_ref, sum_ref, parts_ref):
    merges = merges_ref.shape[1]
    clades = merges + 1

    def over_rates(op, x):
        x = op(x, pltpu.roll(x, 2, 0))
        return op(x, pltpu.roll(x, 4, 0))

    scale = jnp.zeros((8, 128), jnp.float32)
    for k in range(clades):
        start = (k - CLADE_FIRST) % clades * 32
        rows = [roots_ref[start + 8 * a : start + 8 * a + 8, :] for a in range(4)]
        top = jnp.maximum(jnp.maximum(rows[0], rows[1]), jnp.maximum(rows[2], rows[3]))
        top = over_rates(jnp.maximum, top)
        scale = scale + top
        for a in range(4):
            parts_ref[k, 8 * a : 8 * a + 8, :] = jnp.exp(rows[a] - top)

    def branch(node):
        part = [parts_ref[node, 8 * b : 8 * b + 8, :] for b in range(4)]
        out = []
        for a in range(4):
            p = [probs_ref[node * 16 + a * 4 + b] for b in range(4)]
            out.append((p[0] * part[0] + p[1] * part[1]) + (p[2] * part[2] + p[3] * part[3]))
        return out

    for j in range(merges):
        u, v = branch(merges_ref[0, j]), branch(merges_ref[1, j])
        q = [u[a] * v[a] for a in range(4)]
        if j < merges - 1:
            top = jnp.maximum(jnp.maximum(q[0], q[1]), jnp.maximum(q[2], q[3]))
            inv = pl.reciprocal(over_rates(jnp.maximum, top), approx=True)
            scale = scale - jnp.log(inv)
            for a in range(4):
                parts_ref[clades + j, 8 * a : 8 * a + 8, :] = q[a] * inv
        else:
            top = over_rates(jnp.maximum, jnp.maximum(jnp.maximum(q[0], q[1]), jnp.maximum(q[2], q[3])))
            inv = pl.reciprocal(top, approx=True)
            scale = scale - jnp.log(inv)
            total = over_rates(jnp.add, ((q[0] + q[1]) + (q[2] + q[3])) * inv)
    loglik = (jnp.log(total * (1.0 / 16.0)) + scale)[0:2, :]
    weighted = weights_ref[...].astype(jnp.float32) * loglik * (1.0 / total_taxa)
    out_ref[...] = weighted
    sum_ref[...] = jnp.broadcast_to(weighted[0:1, :] + weighted[1:2, :], sum_ref.shape)


def sum_over(rows, axis, first, copies):
    got = all_to_all(rows, axis, first)
    return jnp.broadcast_to(jnp.sum(got, axis=0, keepdims=True), (copies,) + got.shape[1:])


def per_device(tips, transition, clade_children, upper_transition, upper_children, pattern_weights):
    leaves, sites = tips.shape
    clades = lax.axis_size(CLADE)
    groups = lax.axis_size(SITE)
    position = lax.axis_index(CLADE)
    piece = sites // clades
    nodes = transition.shape[0]
    vmem = pl.BlockSpec(memory_space=pltpu.VMEM)
    smem = pl.BlockSpec(memory_space=pltpu.SMEM)

    tiled = tips.reshape(leaves // 8, 8, sites // 128, 128).transpose(0, 2, 1, 3)
    tiled = tiled.reshape(leaves * sites // 128, 128)
    rows = transition.transpose(1, 2, 3, 0).reshape(64, -1)
    hbm = pl.BlockSpec(memory_space=pl.ANY)
    merges = clade_children.T
    logs = pl.pallas_call(
        clade_kernel,
        out_shape=jax.ShapeDtypeStruct((clades * 32, 128), jnp.float32),
        in_specs=[hbm, hbm, hbm],
        out_specs=hbm,
        scratch_shapes=[
            pltpu.SMEM(merges.shape, jnp.int32),
            pltpu.SMEM((2, leaves), jnp.int32),
            pltpu.SMEM(rows.shape, jnp.float32),
            pltpu.VMEM(rows.shape, jnp.float32),
            pltpu.VMEM(tiled.shape, jnp.int32),
            pltpu.VMEM((leaves * 16, 8, 128), jnp.float32),
            pltpu.VMEM(((leaves - 1) * 16, sites // 128, 128), jnp.float32),
            pltpu.VMEM((leaves - 1, sites // 128, 128), jnp.float32),
            pltpu.VMEM((sites // 128, 128), jnp.float32),
            pltpu.VMEM((clades * 32, 128), jnp.float32),
            pltpu.SemaphoreType.DMA((6,)),
        ],
        name="clade",
    )(merges, rows, tiled)

    got = all_to_all(logs.reshape(clades, 32, 128), CLADE, CLADE_FIRST)
    upper_rows = upper_transition.transpose(1, 2, 3, 0).reshape(64, -1)
    spread = pl.pallas_call(
        spread_kernel,
        out_shape=jax.ShapeDtypeStruct((upper_rows.shape[1] * 16, 8, 128), jnp.float32),
        in_specs=[vmem],
        out_specs=vmem,
        compiler_params=pltpu.CompilerParams(vmem_limit_bytes=8 << 20),
        cost_estimate=pl.CostEstimate(flops=1 << 22, bytes_accessed=2 << 20, transcendentals=0),
        name="spread",
    )(upper_rows)
    own = lax.dynamic_slice_in_dim(pattern_weights, position * piece, piece, 0)
    weighted, addend = pl.pallas_call(
        lambda *refs: upper_kernel(float(leaves * clades), *refs),
        out_shape=[
            jax.ShapeDtypeStruct((piece // 128, 128), jnp.float32),
            jax.ShapeDtypeStruct((clades, 128), jnp.float32),
        ],
        in_specs=[smem, vmem, vmem, vmem],
        out_specs=[vmem, vmem],
        scratch_shapes=[pltpu.VMEM((2 * clades - 1, 32, 128), jnp.float32)],
        compiler_params=pltpu.CompilerParams(vmem_limit_bytes=8 << 20),
        name="upper",
    )(upper_children.T, got.reshape(clades * 32, 128), spread, own.reshape(piece // 128, 128))

    part = sum_over(addend.reshape(clades, 1, 128), CLADE, CLADE_FIRST, groups)
    whole = sum_over(part, SITE, SITE_FIRST, 1)
    return weighted.reshape(piece), jnp.sum(whole) / (sites * groups)


def solution(mesh):
    torus = Mesh(mesh.devices.reshape(32, 16), SITE_CLADE)
    return jax.shard_map(
        per_device,
        mesh=torus,
        in_specs=(P(CLADE, SITE), P(CLADE, None, None, None), P(CLADE, None), P(), P(), P(SITE)),
        out_specs=(P(SITE_CLADE), P()),
        check_vma=False,
    )
```

```python
import jax
import jax.numpy as jnp
from jax import lax
from jax.experimental import pallas as pl
from jax.experimental.pallas import tpu as pltpu
from jax.sharding import Mesh
from jax.sharding import PartitionSpec as P

CLADE = "clade"
SITE = "site"
SITE_CLADE = (SITE, CLADE)
CLADE_FIRST = 9
SUM_FIRST = 9
SITE_FIRST = 21


def all_to_all(blocks, axis, first):
    members = lax.axis_size(axis)
    group = [(first + i) % members for i in range(members)]
    return lax.all_to_all(
        blocks, axis, split_axis=0, concat_axis=0, axis_index_groups=[group], tiled=True
    )


def splat(column_block, k):
    return jnp.broadcast_to(column_block[:, k : k + 1], (8, 128))


def by_row(rows):
    shape = (8, rows[0].shape[1])
    sublane = lax.broadcasted_iota(jnp.int32, shape, 0)
    block = jnp.broadcast_to(rows[-1], shape)
    for s in reversed(range(len(rows) - 1)):
        block = jnp.where(sublane <= s, jnp.broadcast_to(rows[s], shape), block)
    return block


def clade_kernel(
    merges_hbm, rows_hbm, tips_hbm, out_hbm,
    merges_ref, order_ref, probs_ref, rows_ref, tips_ref, tables_ref, parts_ref, top_ref, log_ref, root_ref, sems,
):
    copies = [
        pltpu.make_async_copy(source, target, sems.at[i])
        for i, (source, target) in enumerate(
            [(rows_hbm, rows_ref), (merges_hbm, merges_ref), (rows_hbm, probs_ref), (tips_hbm, tips_ref)]
        )
    ]
    for copy in copies:
        copy.start()
    merges = merges_ref.shape[1]
    leaves = merges + 1
    groups = out_hbm.shape[0] // 32
    tiles = range(2 * groups // 8)
    log_ref[...] = jnp.zeros_like(log_ref)
    copies[0].wait()
    copies[1].wait()
    blocks = []
    for k in range(16):
        rows = [rows_ref[4 * k + b : 4 * k + b + 1, :] for b in range(4)]
        blocks.append(by_row(rows + [(rows[0] + rows[1]) + (rows[2] + rows[3])]))
    for taxon in range(leaves):
        for k in range(16):
            tables_ref[taxon * 16 + k] = splat(blocks[k], taxon)
    pairs, others = jnp.int32(0), jnp.int32(0)
    for j in range(merges):
        is_pair = jnp.maximum(merges_ref[0, j], merges_ref[1, j]) < leaves
        order_ref[0, pairs] = j
        order_ref[1, others] = j
        pairs = pairs + jnp.where(is_pair, 1, 0)
        others = others + jnp.where(is_pair, 0, 1)
    copies[3].wait()

    def codes(taxon):
        start = (taxon // 8) * (16 * groups) + taxon % 8
        halves = [tips_ref[pl.ds(start + 8 * h, groups, stride=16), :] for h in range(2)]
        return [half[8 * i : 8 * i + 8] for half in halves for i in range(groups // 8)]

    def leaf_branch(taxon):
        idx = codes(taxon)

        def planes(rate):
            for state in range(4):
                column = tables_ref[taxon * 16 + rate * 4 + state]
                yield [
                    jnp.take_along_axis(column, idx[t], axis=0, mode="promise_in_bounds")
                    for t in tiles
                ]

        return planes

    def add_logs(invs):
        for t in tiles:
            rows = slice(8 * t, 8 * t + 8)
            log_ref[rows, :] = log_ref[rows, :] - sum(jnp.log(inv[t]) for inv in invs)

    def inner_branch(node):
        inner = node - leaves
        inv = [
            pl.reciprocal(top_ref[inner, 8 * t : 8 * t + 8, :], approx=True) for t in tiles
        ]

        def planes(rate):
            part = [
                [
                    parts_ref[inner * 16 + rate * 4 + b, 8 * t : 8 * t + 8, :] * inv[t]
                    for t in tiles
                ]
                for b in range(4)
            ]
            for state in range(4):
                p = [probs_ref[rate * 16 + state * 4 + b, node] for b in range(4)]
                yield [
                    (p[0] * part[0][t] + p[1] * part[1][t])
                    + (p[2] * part[2][t] + p[3] * part[3][t])
                    for t in tiles
                ]

        planes.inv = inv
        return planes

    def merge(j, one, other):
        add_logs_of = [branch.inv for branch in (one, other) if hasattr(branch, "inv")]
        if add_logs_of:
            add_logs(add_logs_of)
        biggest = None
        for rate in range(4):
            firsts = list(one(rate))
            for state, (u, v) in enumerate(zip(firsts, other(rate))):
                q = [u[t] * v[t] for t in tiles]
                for t in tiles:
                    parts_ref[j * 16 + rate * 4 + state, 8 * t : 8 * t + 8, :] = q[t]
                biggest = q if biggest is None else [jnp.maximum(biggest[t], q[t]) for t in tiles]
        for t in tiles:
            top_ref[j, 8 * t : 8 * t + 8, :] = biggest[t]

    def two_pairs(i, _):
        for place in (2 * i, jnp.minimum(2 * i + 1, pairs - 1)):
            j = order_ref[0, place]
            merge(j, leaf_branch(merges_ref[0, j]), leaf_branch(merges_ref[1, j]))
        return 0

    def step(i, _):
        j = order_ref[1, i]
        c, d = merges_ref[0, j], merges_ref[1, j]
        high, low = jnp.maximum(c, d), jnp.minimum(c, d)
        leaf, inner = leaf_branch, inner_branch
        pl.when(low < leaves)(lambda: merge(j, inner(high), leaf(low)))
        pl.when(low >= leaves)(lambda: merge(j, inner(high), inner(low)))
        return 0

    lax.fori_loop(0, (pairs + 1) // 2, two_pairs, 0)
    copies[2].wait()
    lax.fori_loop(0, others, step, 0)

    last = merges - 1
    runs = [(0, CLADE_FIRST, groups - CLADE_FIRST), (CLADE_FIRST, groups, 0)]
    sends = []
    for part in range(groups // 8):
        for h in range(2):
            rows = slice(h * groups + 8 * part, h * groups + 8 * part + 8)
            scale = log_ref[rows, :]
            for rate in range(4):
                for state in range(4):
                    value = jnp.log(parts_ref[last * 16 + rate * 4 + state, rows, :]) + scale
                    start = part * 256 + state * 8 + rate * 2 + h
                    root_ref[pl.ds(start, 8, stride=32), :] = value
        while len(sends) < 2 and runs[len(sends)][1] <= 8 * part + 8:
            low, high, place = runs[len(sends)]
            span = pl.ds(low * 32, (high - low) * 32)
            target = pl.ds(place * 32, (high - low) * 32)
            sends.append(
                pltpu.make_async_copy(root_ref.at[span], out_hbm.at[target], sems.at[4 + len(sends)])
            )
            sends[-1].start()
    for send in sends:
        send.wait()


def spread_kernel(rows_ref, out_ref):
    for k in range(16):
        rows = [rows_ref[16 * rate + k : 16 * rate + k + 1, :] for rate in range(4)]
        block = by_row([row for row in rows for _ in range(2)])
        for node in range(rows_ref.shape[1]):
            out_ref[node * 16 + k] = splat(block, node)


def upper_kernel(total_taxa, merges_ref, roots_ref, probs_ref, weights_ref, out_ref, sum_ref, parts_ref):
    merges = merges_ref.shape[1]
    clades = merges + 1

    def over_rates(op, x):
        x = op(x, pltpu.roll(x, 2, 0))
        return op(x, pltpu.roll(x, 4, 0))

    scale = jnp.zeros((8, 128), jnp.float32)
    for k in range(clades):
        start = (k - CLADE_FIRST) % clades * 32
        rows = [roots_ref[start + 8 * a : start + 8 * a + 8, :] for a in range(4)]
        top = jnp.maximum(jnp.maximum(rows[0], rows[1]), jnp.maximum(rows[2], rows[3]))
        top = over_rates(jnp.maximum, top)
        scale = scale + top
        for a in range(4):
            parts_ref[k, 8 * a : 8 * a + 8, :] = jnp.exp(rows[a] - top)

    def branch(node):
        part = [parts_ref[node, 8 * b : 8 * b + 8, :] for b in range(4)]
        out = []
        for a in range(4):
            p = [probs_ref[node * 16 + a * 4 + b] for b in range(4)]
            out.append((p[0] * part[0] + p[1] * part[1]) + (p[2] * part[2] + p[3] * part[3]))
        return out

    for j in range(merges):
        u, v = branch(merges_ref[0, j]), branch(merges_ref[1, j])
        q = [u[a] * v[a] for a in range(4)]
        if j < merges - 1:
            top = jnp.maximum(jnp.maximum(q[0], q[1]), jnp.maximum(q[2], q[3]))
            inv = pl.reciprocal(over_rates(jnp.maximum, top), approx=True)
            scale = scale - jnp.log(inv)
            for a in range(4):
                parts_ref[clades + j, 8 * a : 8 * a + 8, :] = q[a] * inv
        else:
            top = over_rates(jnp.maximum, jnp.maximum(jnp.maximum(q[0], q[1]), jnp.maximum(q[2], q[3])))
            inv = pl.reciprocal(top, approx=True)
            scale = scale - jnp.log(inv)
            total = over_rates(jnp.add, ((q[0] + q[1]) + (q[2] + q[3])) * inv)
    loglik = (jnp.log(total * (1.0 / 16.0)) + scale)[0:2, :]
    weighted = weights_ref[...].astype(jnp.float32) * loglik * (1.0 / total_taxa)
    out_ref[...] = weighted
    sum_ref[...] = jnp.broadcast_to(weighted[0:1, :] + weighted[1:2, :], sum_ref.shape)


def finish_kernel(total_sites, parts_ref, weighted_ref, out_ref, mean_ref):
    out_ref[...] = weighted_ref[...]
    by_lane = jnp.sum(parts_ref[...], axis=0, keepdims=True)
    mean_ref[...] = jnp.sum(by_lane, axis=1, keepdims=True) * (1.0 / total_sites)


def sum_over(rows, axis, first, copies):
    got = all_to_all(rows, axis, first)
    return jnp.broadcast_to(jnp.sum(got, axis=0, keepdims=True), (copies,) + got.shape[1:])


def per_device(tips, transition, clade_children, upper_transition, upper_children, pattern_weights):
    leaves, sites = tips.shape
    clades = lax.axis_size(CLADE)
    groups = lax.axis_size(SITE)
    position = lax.axis_index(CLADE)
    piece = sites // clades
    nodes = transition.shape[0]
    vmem = pl.BlockSpec(memory_space=pltpu.VMEM)
    smem = pl.BlockSpec(memory_space=pltpu.SMEM)

    tiled = tips.reshape(leaves // 8, 8, sites // 128, 128).transpose(0, 2, 1, 3)
    tiled = tiled.reshape(leaves * sites // 128, 128)
    rows = transition.transpose(1, 2, 3, 0).reshape(64, -1)
    hbm = pl.BlockSpec(memory_space=pl.ANY)
    merges = clade_children.T
    logs = pl.pallas_call(
        clade_kernel,
        out_shape=jax.ShapeDtypeStruct((clades * 32, 128), jnp.float32),
        in_specs=[hbm, hbm, hbm],
        out_specs=hbm,
        scratch_shapes=[
            pltpu.SMEM(merges.shape, jnp.int32),
            pltpu.SMEM((2, leaves), jnp.int32),
            pltpu.SMEM(rows.shape, jnp.float32),
            pltpu.VMEM(rows.shape, jnp.float32),
            pltpu.VMEM(tiled.shape, jnp.int32),
            pltpu.VMEM((leaves * 16, 8, 128), jnp.float32),
            pltpu.VMEM(((leaves - 1) * 16, sites // 128, 128), jnp.float32),
            pltpu.VMEM((leaves - 1, sites // 128, 128), jnp.float32),
            pltpu.VMEM((sites // 128, 128), jnp.float32),
            pltpu.VMEM((clades * 32, 128), jnp.float32),
            pltpu.SemaphoreType.DMA((6,)),
        ],
        name="clade",
    )(merges, rows, tiled)

    got = all_to_all(logs.reshape(clades, 32, 128), CLADE, CLADE_FIRST)
    upper_rows = upper_transition.transpose(1, 2, 3, 0).reshape(64, -1)
    spread = pl.pallas_call(
        spread_kernel,
        out_shape=jax.ShapeDtypeStruct((upper_rows.shape[1] * 16, 8, 128), jnp.float32),
        in_specs=[vmem],
        out_specs=vmem,
        compiler_params=pltpu.CompilerParams(vmem_limit_bytes=8 << 20),
        cost_estimate=pl.CostEstimate(flops=1 << 22, bytes_accessed=2 << 20, transcendentals=0),
        name="spread",
    )(upper_rows)
    own = lax.dynamic_slice_in_dim(pattern_weights, position * piece, piece, 0)
    weighted, addend = pl.pallas_call(
        lambda *refs: upper_kernel(float(leaves * clades), *refs),
        out_shape=[
            jax.ShapeDtypeStruct((piece // 128, 128), jnp.float32),
            jax.ShapeDtypeStruct((clades, 128), jnp.float32),
        ],
        in_specs=[smem, vmem, vmem, vmem],
        out_specs=[vmem, vmem],
        scratch_shapes=[pltpu.VMEM((2 * clades - 1, 32, 128), jnp.float32)],
        compiler_params=pltpu.CompilerParams(vmem_limit_bytes=8 << 20),
        name="upper",
    )(upper_children.T, got.reshape(clades * 32, 128), spread, own.reshape(piece // 128, 128))

    part = sum_over(addend.reshape(clades, 1, 128), CLADE, SUM_FIRST, groups)
    whole = all_to_all(part, SITE, SITE_FIRST).reshape(groups, 128)
    weighted, mean = pl.pallas_call(
        lambda *refs: finish_kernel(float(sites * groups), *refs),
        out_shape=[
            jax.ShapeDtypeStruct(weighted.shape, jnp.float32),
            jax.ShapeDtypeStruct((1, 1), jnp.float32),
        ],
        in_specs=[vmem, vmem],
        out_specs=[vmem, vmem],
        compiler_params=pltpu.CompilerParams(vmem_limit_bytes=4 << 20),
        name="finish",
    )(whole, weighted)
    return weighted.reshape(piece), mean.reshape(())


def solution(mesh):
    torus = Mesh(mesh.devices.reshape(32, 16), SITE_CLADE)
    return jax.shard_map(
        per_device,
        mesh=torus,
        in_specs=(P(CLADE, SITE), P(CLADE, None, None, None), P(CLADE, None), P(), P(), P(SITE)),
        out_specs=(P(SITE_CLADE), P()),
        check_vma=False,
    )
```

```python
import jax
import jax.numpy as jnp
from jax import lax
from jax.experimental import pallas as pl
from jax.experimental.pallas import tpu as pltpu
from jax.sharding import Mesh
from jax.sharding import PartitionSpec as P

CLADE = "clade"
SITE = "site"
SITE_CLADE = (SITE, CLADE)
CLADE_FIRST = 9
SUM_FIRST = 9
SITE_FIRST = 21


def all_to_all(blocks, axis, first):
    members = lax.axis_size(axis)
    group = [(first + i) % members for i in range(members)]
    return lax.all_to_all(
        blocks, axis, split_axis=0, concat_axis=0, axis_index_groups=[group], tiled=True
    )


def splat(column_block, k):
    return jnp.broadcast_to(column_block[:, k : k + 1], (8, 128))


def by_row(rows):
    shape = (8, rows[0].shape[1])
    sublane = lax.broadcasted_iota(jnp.int32, shape, 0)
    block = jnp.broadcast_to(rows[-1], shape)
    for s in reversed(range(len(rows) - 1)):
        block = jnp.where(sublane <= s, jnp.broadcast_to(rows[s], shape), block)
    return block


def clade_kernel(
    merges_hbm, rows_hbm, tips_hbm, out_hbm,
    merges_ref, order_ref, probs_ref, rows_ref, tips_ref, tables_ref, parts_ref, top_ref, log_ref, root_ref, sems,
):
    copies = [
        pltpu.make_async_copy(source, target, sems.at[i])
        for i, (source, target) in enumerate(
            [(rows_hbm, rows_ref), (merges_hbm, merges_ref), (rows_hbm, probs_ref), (tips_hbm, tips_ref)]
        )
    ]
    for copy in copies:
        copy.start()
    merges = merges_ref.shape[1]
    leaves = merges + 1
    groups = out_hbm.shape[0] // 32
    tiles = range(2 * groups // 8)
    log_ref[...] = jnp.zeros_like(log_ref)
    copies[0].wait()
    copies[1].wait()
    blocks = []
    for k in range(16):
        rows = [rows_ref[4 * k + b : 4 * k + b + 1, :] for b in range(4)]
        blocks.append(by_row(rows + [(rows[0] + rows[1]) + (rows[2] + rows[3])]))
    for taxon in range(leaves):
        for k in range(16):
            tables_ref[taxon * 16 + k] = splat(blocks[k], taxon)
    pairs, others = jnp.int32(0), jnp.int32(0)
    for j in range(merges):
        is_pair = jnp.maximum(merges_ref[0, j], merges_ref[1, j]) < leaves
        order_ref[0, pairs] = j
        order_ref[1, others] = j
        pairs = pairs + jnp.where(is_pair, 1, 0)
        others = others + jnp.where(is_pair, 0, 1)
    copies[3].wait()

    def codes(taxon):
        start = (taxon // 8) * (16 * groups) + taxon % 8
        halves = [tips_ref[pl.ds(start + 8 * h, groups, stride=16), :] for h in range(2)]
        return [half[8 * i : 8 * i + 8] for half in halves for i in range(groups // 8)]

    def leaf_branch(taxon):
        idx = codes(taxon)

        def planes(rate):
            for state in range(4):
                column = tables_ref[taxon * 16 + rate * 4 + state]
                yield [
                    jnp.take_along_axis(column, idx[t], axis=0, mode="promise_in_bounds")
                    for t in tiles
                ]

        return planes

    def add_logs(invs):
        for t in tiles:
            rows = slice(8 * t, 8 * t + 8)
            log_ref[rows, :] = log_ref[rows, :] - sum(jnp.log(inv[t]) for inv in invs)

    def inner_branch(node):
        inner = node - leaves
        inv = [
            pl.reciprocal(top_ref[inner, 8 * t : 8 * t + 8, :], approx=True) for t in tiles
        ]

        def planes(rate):
            part = [
                [
                    parts_ref[inner * 16 + rate * 4 + b, 8 * t : 8 * t + 8, :] * inv[t]
                    for t in tiles
                ]
                for b in range(4)
            ]
            for state in range(4):
                p = [probs_ref[rate * 16 + state * 4 + b, node] for b in range(4)]
                yield [
                    (p[0] * part[0][t] + p[1] * part[1][t])
                    + (p[2] * part[2][t] + p[3] * part[3][t])
                    for t in tiles
                ]

        planes.inv = inv
        return planes

    def merge(j, one, other):
        add_logs_of = [branch.inv for branch in (one, other) if hasattr(branch, "inv")]
        if add_logs_of:
            add_logs(add_logs_of)
        biggest = None
        for rate in range(4):
            firsts = list(one(rate))
            for state, (u, v) in enumerate(zip(firsts, other(rate))):
                q = [u[t] * v[t] for t in tiles]
                for t in tiles:
                    parts_ref[j * 16 + rate * 4 + state, 8 * t : 8 * t + 8, :] = q[t]
                biggest = q if biggest is None else [jnp.maximum(biggest[t], q[t]) for t in tiles]
        for t in tiles:
            top_ref[j, 8 * t : 8 * t + 8, :] = biggest[t]

    def two_pairs(i, _):
        for place in (2 * i, jnp.minimum(2 * i + 1, pairs - 1)):
            j = order_ref[0, place]
            merge(j, leaf_branch(merges_ref[0, j]), leaf_branch(merges_ref[1, j]))
        return 0

    def fetch(i):
        j = order_ref[1, i]
        c, d = merges_ref[0, j], merges_ref[1, j]
        return j, jnp.maximum(c, d), jnp.minimum(c, d)

    def step(i, now):
        j, high, low = now
        later = fetch(jnp.minimum(i + 1, others - 1))
        leaf, inner = leaf_branch, inner_branch
        lax.cond(
            low < leaves,
            lambda: merge(j, inner(high), leaf(low)),
            lambda: merge(j, inner(high), inner(low)),
        )
        return later

    lax.fori_loop(0, (pairs + 1) // 2, two_pairs, 0)
    copies[2].wait()
    lax.fori_loop(0, others, step, fetch(0))

    last = merges - 1
    runs = [(0, CLADE_FIRST, groups - CLADE_FIRST), (CLADE_FIRST, groups, 0)]
    sends = []
    for part in range(groups // 8):
        for h in range(2):
            rows = slice(h * groups + 8 * part, h * groups + 8 * part + 8)
            scale = log_ref[rows, :]
            for rate in range(4):
                for state in range(4):
                    value = jnp.log(parts_ref[last * 16 + rate * 4 + state, rows, :]) + scale
                    start = part * 256 + state * 8 + rate * 2 + h
                    root_ref[pl.ds(start, 8, stride=32), :] = value
        while len(sends) < 2 and runs[len(sends)][1] <= 8 * part + 8:
            low, high, place = runs[len(sends)]
            span = pl.ds(low * 32, (high - low) * 32)
            target = pl.ds(place * 32, (high - low) * 32)
            sends.append(
                pltpu.make_async_copy(root_ref.at[span], out_hbm.at[target], sems.at[4 + len(sends)])
            )
            sends[-1].start()
    for send in sends:
        send.wait()


def spread_kernel(rows_ref, out_ref):
    for k in range(16):
        rows = [rows_ref[16 * rate + k : 16 * rate + k + 1, :] for rate in range(4)]
        block = by_row([row for row in rows for _ in range(2)])
        for node in range(rows_ref.shape[1]):
            out_ref[node * 16 + k] = splat(block, node)


def upper_kernel(total_taxa, merges_ref, roots_ref, probs_ref, weights_ref, out_ref, sum_ref, parts_ref):
    merges = merges_ref.shape[1]
    clades = merges + 1

    def over_rates(op, x):
        x = op(x, pltpu.roll(x, 2, 0))
        return op(x, pltpu.roll(x, 4, 0))

    scale = jnp.zeros((8, 128), jnp.float32)
    for k in range(clades):
        start = (k - CLADE_FIRST) % clades * 32
        rows = [roots_ref[start + 8 * a : start + 8 * a + 8, :] for a in range(4)]
        top = jnp.maximum(jnp.maximum(rows[0], rows[1]), jnp.maximum(rows[2], rows[3]))
        top = over_rates(jnp.maximum, top)
        scale = scale + top
        for a in range(4):
            parts_ref[k, 8 * a : 8 * a + 8, :] = jnp.exp(rows[a] - top)

    def branch(node):
        part = [parts_ref[node, 8 * b : 8 * b + 8, :] for b in range(4)]
        out = []
        for a in range(4):
            p = [probs_ref[node * 16 + a * 4 + b] for b in range(4)]
            out.append((p[0] * part[0] + p[1] * part[1]) + (p[2] * part[2] + p[3] * part[3]))
        return out

    for j in range(merges):
        u, v = branch(merges_ref[0, j]), branch(merges_ref[1, j])
        q = [u[a] * v[a] for a in range(4)]
        if j < merges - 1:
            top = jnp.maximum(jnp.maximum(q[0], q[1]), jnp.maximum(q[2], q[3]))
            inv = pl.reciprocal(over_rates(jnp.maximum, top), approx=True)
            scale = scale - jnp.log(inv)
            for a in range(4):
                parts_ref[clades + j, 8 * a : 8 * a + 8, :] = q[a] * inv
        else:
            top = over_rates(jnp.maximum, jnp.maximum(jnp.maximum(q[0], q[1]), jnp.maximum(q[2], q[3])))
            inv = pl.reciprocal(top, approx=True)
            scale = scale - jnp.log(inv)
            total = over_rates(jnp.add, ((q[0] + q[1]) + (q[2] + q[3])) * inv)
    loglik = (jnp.log(total * (1.0 / 16.0)) + scale)[0:2, :]
    weighted = weights_ref[...].astype(jnp.float32) * loglik * (1.0 / total_taxa)
    out_ref[...] = weighted
    sum_ref[...] = jnp.broadcast_to(weighted[0:1, :] + weighted[1:2, :], sum_ref.shape)


def finish_kernel(total_sites, parts_ref, weighted_ref, out_ref, mean_ref):
    out_ref[...] = weighted_ref[...]
    by_lane = jnp.sum(parts_ref[...], axis=0, keepdims=True)
    mean_ref[...] = jnp.sum(by_lane, axis=1, keepdims=True) * (1.0 / total_sites)


def sum_over(rows, axis, first, copies):
    got = all_to_all(rows, axis, first)
    return jnp.broadcast_to(jnp.sum(got, axis=0, keepdims=True), (copies,) + got.shape[1:])


def per_device(tips, transition, clade_children, upper_transition, upper_children, pattern_weights):
    leaves, sites = tips.shape
    clades = lax.axis_size(CLADE)
    groups = lax.axis_size(SITE)
    position = lax.axis_index(CLADE)
    piece = sites // clades
    nodes = transition.shape[0]
    vmem = pl.BlockSpec(memory_space=pltpu.VMEM)
    smem = pl.BlockSpec(memory_space=pltpu.SMEM)

    tiled = tips.reshape(leaves // 8, 8, sites // 128, 128).transpose(0, 2, 1, 3)
    tiled = tiled.reshape(leaves * sites // 128, 128)
    rows = transition.transpose(1, 2, 3, 0).reshape(64, -1)
    hbm = pl.BlockSpec(memory_space=pl.ANY)
    merges = clade_children.T
    logs = pl.pallas_call(
        clade_kernel,
        out_shape=jax.ShapeDtypeStruct((clades * 32, 128), jnp.float32),
        in_specs=[hbm, hbm, hbm],
        out_specs=hbm,
        scratch_shapes=[
            pltpu.SMEM(merges.shape, jnp.int32),
            pltpu.SMEM((2, leaves), jnp.int32),
            pltpu.SMEM(rows.shape, jnp.float32),
            pltpu.VMEM(rows.shape, jnp.float32),
            pltpu.VMEM(tiled.shape, jnp.int32),
            pltpu.VMEM((leaves * 16, 8, 128), jnp.float32),
            pltpu.VMEM(((leaves - 1) * 16, sites // 128, 128), jnp.float32),
            pltpu.VMEM((leaves - 1, sites // 128, 128), jnp.float32),
            pltpu.VMEM((sites // 128, 128), jnp.float32),
            pltpu.VMEM((clades * 32, 128), jnp.float32),
            pltpu.SemaphoreType.DMA((6,)),
        ],
        compiler_params=pltpu.CompilerParams(),
        name="clade",
    )(merges, rows, tiled)

    got = all_to_all(logs.reshape(clades, 32, 128), CLADE, CLADE_FIRST)
    upper_rows = upper_transition.transpose(1, 2, 3, 0).reshape(64, -1)
    spread = pl.pallas_call(
        spread_kernel,
        out_shape=jax.ShapeDtypeStruct((upper_rows.shape[1] * 16, 8, 128), jnp.float32),
        in_specs=[vmem],
        out_specs=vmem,
        compiler_params=pltpu.CompilerParams(vmem_limit_bytes=8 << 20),
        cost_estimate=pl.CostEstimate(flops=1 << 22, bytes_accessed=2 << 20, transcendentals=0),
        name="spread",
    )(upper_rows)
    own = lax.dynamic_slice_in_dim(pattern_weights, position * piece, piece, 0)
    weighted, addend = pl.pallas_call(
        lambda *refs: upper_kernel(float(leaves * clades), *refs),
        out_shape=[
            jax.ShapeDtypeStruct((piece // 128, 128), jnp.float32),
            jax.ShapeDtypeStruct((clades, 128), jnp.float32),
        ],
        in_specs=[smem, vmem, vmem, vmem],
        out_specs=[vmem, vmem],
        scratch_shapes=[pltpu.VMEM((2 * clades - 1, 32, 128), jnp.float32)],
        compiler_params=pltpu.CompilerParams(vmem_limit_bytes=8 << 20),
        name="upper",
    )(upper_children.T, got.reshape(clades * 32, 128), spread, own.reshape(piece // 128, 128))

    part = sum_over(addend.reshape(clades, 1, 128), CLADE, SUM_FIRST, groups)
    whole = all_to_all(part, SITE, SITE_FIRST).reshape(groups, 128)
    weighted, mean = pl.pallas_call(
        lambda *refs: finish_kernel(float(sites * groups), *refs),
        out_shape=[
            jax.ShapeDtypeStruct(weighted.shape, jnp.float32),
            jax.ShapeDtypeStruct((1, 1), jnp.float32),
        ],
        in_specs=[vmem, vmem],
        out_specs=[vmem, vmem],
        compiler_params=pltpu.CompilerParams(vmem_limit_bytes=4 << 20),
        name="finish",
    )(whole, weighted)
    return weighted.reshape(piece), mean.reshape(())


def solution(mesh):
    torus = Mesh(mesh.devices.reshape(32, 16), SITE_CLADE)
    return jax.shard_map(
        per_device,
        mesh=torus,
        in_specs=(P(CLADE, SITE), P(CLADE, None, None, None), P(CLADE, None), P(), P(), P(SITE)),
        out_specs=(P(SITE_CLADE), P()),
        check_vma=False,
    )
```
